32 devices in a mesh: clip: 2 (over y), tm: 4 (over z), space: 2 (over x), chan: 2 (over core).
Axes of the slice: x: 2, y: 2, z: 4, core: 2. Of those that a mesh axis runs over, the one named last changes fastest.
Arguments:
- features: bfloat16 [16, 8, 90, 256], P(('clip', 'tm'), 'space'), parts along dimension 0, may hold values from -700 to 700
- hidden: bfloat16 [16, 8, 90, 256], P(('clip', 'tm'), 'space'), parts along dimension 0, may hold values from -700 to 700
- cotangent: bfloat16 [16, 8, 90, 256], P(('clip', 'tm'), 'space'), parts along dimension 0, may hold values from -6 to 6
- kernel_one: bfloat16 [256, 3, 3, 3, 256], P(None, None, None, None, 'chan'), may hold values from -0.078125 to 0.078125
- kernel_two: bfloat16 [256, 3, 3, 3, 256], P(None, None, None, None, 'chan'), may hold values from -0.078125 to 0.078125
- gains: float32 [2, 256], replicated, may hold values from 0.25 to 1.75
Outputs:
- feature_grad: bfloat16 [16, 8, 90, 256], P(('clip', 'tm'), 'space', None, 'chan'), parts along dimension 0
- delta_one: float32 [512, 3, 3, 3, 256], P(('clip', 'tm', 'space'), None, None, None, 'chan'), parts along dimension 0
- delta_two: float32 [512, 3, 3, 3, 256], P(('clip', 'tm', 'space'), None, None, None, 'chan'), parts along dimension 0
- gain_grads: float32 [4, 256], P('clip', 'chan'), parts along dimension 0
The draws below stay inside these ranges and needn't reach their ends.
There are 2 independent parts, one for each index of `clip`. The reference program is written for one: setup_inputs(seed, part) draws one part's arguments, and reference() takes and returns one part's arrays. A program takes and returns all parts, laid end to end along the dimension named above; an argument that names none is the same for every part. Nothing has to cross between parts.
All inputs are finite; a program needn't handle non-finite values.
Results may differ from the reference program's by a relative error of at most 0.005.
Values may be sent and summed in bfloat16 or wider, within the bound.
No kernel may reach another device: no remote copies, remote signals or barrier semaphores. Data moves between devices by JAX's collectives and lax.ppermute only.
A program may use at most 128 MiB of HBM per device.

```python
import math
import jax
import jax.numpy as jnp
from jax import lax

C = 256
GROUPS = 32
W = 90
FRAMES = 8
HEIGHT = 8


def field_draw(key):
    key_base, key_rows, key_chan = jax.random.split(key, 3)
    shape = (FRAMES, HEIGHT, W, C)
    row_scale = 0.2 * jnp.exp(jax.random.uniform(key_rows, (FRAMES, HEIGHT, 1, 1), jnp.float32, 0.0, math.log(10.0)))
    chan_scale = jnp.exp(jax.random.uniform(key_chan, (1, 1, 1, C), jnp.float32, 0.0, math.log(4.0)))
    position = jnp.arange(FRAMES, dtype=jnp.float32).reshape(FRAMES, 1, 1, 1) / max(FRAMES - 1, 1)
    base = jnp.clip(jax.random.normal(key_base, shape, jnp.float32), -4.0, 4.0)
    rise = jnp.exp(0.5 * math.log(3.0) * position)
    return base * row_scale * chan_scale * rise


def draw_features(key, part):
    return field_draw(jax.random.fold_in(key, 11)).astype(jnp.bfloat16)


def draw_hidden(key, part):
    return field_draw(jax.random.fold_in(key, 23)).astype(jnp.bfloat16)


def block_levels(rng, shape, cuts, least, high):
    loudness, own = 1.0, jax.random.fold_in(rng, 6)
    for dim, blocks in cuts:
        heights = jnp.exp(jax.random.uniform(jax.random.fold_in(own, dim), (blocks,), jnp.float32, least / len(cuts), high / len(cuts)))
        loudness = loudness * jnp.repeat(heights, shape[dim] // blocks).reshape([-1 if axis == dim else 1 for axis in range(len(shape))])
    return loudness


def scatter_about(stream_key, extent, deviation, bound, cuts=(), kind=jnp.bfloat16):
    entries = deviation * jax.random.normal(stream_key, extent, jnp.float32)
    if cuts:
        entries = entries * block_levels(stream_key, extent, cuts, -0.22, 0.18)
    return jnp.clip(entries, -bound, bound).astype(kind)


def setup_inputs(seed: int = 0, part: int = 0) -> dict:
    streams_of = jax.random.split(jax.random.key(seed), 7)
    part_splits = jax.random.split(jax.random.fold_in(streams_of[6], part), 7)
    features = draw_features(jax.random.fold_in(jax.random.fold_in(streams_of[6], part), 71), part)
    hidden = draw_hidden(jax.random.fold_in(jax.random.fold_in(streams_of[6], part), 71), part)
    cotangent = scatter_about(part_splits[2], (FRAMES, HEIGHT, W, C), 1.0, 6.0, ((0, 4), (1, 2)))
    kernel_one = scatter_about(streams_of[3], (C, 3, 3, 3, C), (27 * C) ** -0.5, 0.078125, ((4, 2),))
    kernel_two = scatter_about(streams_of[4], (C, 3, 3, 3, C), (27 * C) ** -0.5, 0.078125, ((4, 2),))
    gains = jnp.clip(1.0 + 0.15 * jax.random.normal(streams_of[5], (2, C), jnp.float32), 0.25, 1.75)
    return dict(features=features, hidden=hidden, cotangent=cotangent, kernel_one=kernel_one, kernel_two=kernel_two, gains=gains)


epsilon = 1e-06

def moments(field, gain, members):
    per = field.shape[3] // GROUPS
    total = lax.optimization_barrier(jnp.sum(field, axis=(0, 1, 2))).reshape(GROUPS, per)
    square = lax.optimization_barrier(jnp.sum(field * field, axis=(0, 1, 2))).reshape(GROUPS, per)
    mean = lax.optimization_barrier(jnp.sum(total, axis=1)) / members
    spread = lax.optimization_barrier(jnp.sum(square, axis=1)) / members - mean * mean
    scale = jnp.repeat(lax.rsqrt(spread + epsilon), per)
    centred = (field - jnp.repeat(mean, per)) * scale
    return (centred, centred * gain, scale)

def norm_back(upstream, centred, scaled, gain, scale, members):
    per = upstream.shape[3] // GROUPS
    gate = jax.nn.sigmoid(scaled)
    slope = upstream * gate * (1.0 + scaled * (1.0 - gate))
    plain = lax.optimization_barrier(jnp.sum(slope, axis=(0, 1, 2)))
    weighted = lax.optimization_barrier(jnp.sum(slope * centred, axis=(0, 1, 2)))
    first = jnp.repeat(lax.optimization_barrier(jnp.sum((gain * plain).reshape(-1, per), axis=1)), per) / members
    second = jnp.repeat(lax.optimization_barrier(jnp.sum((gain * weighted).reshape(-1, per), axis=1)), per) / members
    return (scale * (slope * gain - first - centred * second), weighted)

def conv_back(active, grad, kernel):
    frames, height, width, channels = active.shape
    padded = jnp.pad(grad.astype(jnp.float32), ((0, 2), (1, 1), (1, 1), (0, 0)))
    flipped = jnp.flip(jnp.transpose(kernel.astype(jnp.float32), (1, 2, 3, 4, 0)), (0, 1, 2))
    back = lax.conv_general_dilated(padded[None], flipped, (1, 1, 1), ((0, 0), (0, 0), (0, 0)), dimension_numbers=('NDHWC', 'DHWIO', 'NDHWC'), precision=lax.Precision.HIGHEST)[0]
    flat = active.reshape(-1, channels).astype(jnp.float32)
    pieces = []
    for frame_tap in range(3):
        for row_tap in range(3):
            for col_tap in range(3):
                window = padded[2 - frame_tap:2 - frame_tap + frames, 2 - row_tap:2 - row_tap + height, 2 - col_tap:2 - col_tap + width].reshape(-1, channels)
                pieces.append(lax.dot_general(flat, window, (((0,), (0,)), ((), ())), precision=lax.Precision.HIGHEST))
    delta = jnp.stack(pieces, axis=1).reshape(channels, 3, 3, 3, channels)
    return (delta, back)

def reference(features, hidden, cotangent, kernel_one, kernel_two, gains):
    members = float(FRAMES * HEIGHT * W * (C // GROUPS))
    centred_one, scaled_one, scale_one = moments(features.astype(jnp.float32), gains[0], members)
    centred_two, scaled_two, scale_two = moments(hidden.astype(jnp.float32), gains[1], members)
    active_one = (scaled_one * jax.nn.sigmoid(scaled_one)).astype(jnp.bfloat16)
    active_two = (scaled_two * jax.nn.sigmoid(scaled_two)).astype(jnp.bfloat16)
    delta_two, back_two = conv_back(active_two, cotangent, kernel_two)
    grad_two, weighted_two = norm_back(back_two, centred_two, scaled_two, gains[1], scale_two, members)
    grad_hidden = grad_two.astype(jnp.bfloat16)
    delta_one, back_one = conv_back(active_one, grad_hidden, kernel_one)
    grad_one, weighted_one = norm_back(back_one, centred_one, scaled_one, gains[0], scale_one, members)
    feature_grad = (cotangent.astype(jnp.float32) + grad_one).astype(jnp.bfloat16)
    return (feature_grad, delta_one, delta_two, jnp.stack([weighted_one, weighted_two]))
```

```python
import jax
import jax.numpy as jnp
from jax import lax
from jax.experimental import pallas as pl
from jax.experimental.pallas import tpu as pltpu
from jax.sharding import PartitionSpec as P

GROUPS = 32


epsilon = 1e-06


CLIP = ("tm", "space")


def clip_totals(values):
    count = lax.axis_size(CLIP)
    if count & (count - 1):
        return lax.psum(values, CLIP)
    step = 1
    while step < count:
        values = values + lax.ppermute(values, CLIP, [(i, i ^ step) for i in range(count)])
        step *= 2
    return values


def statistics(total, square, members, per):
    mean = jnp.sum(total.reshape(-1, per), axis=1) / members
    spread = jnp.sum(square.reshape(-1, per), axis=1) / members - mean * mean
    scale = lax.rsqrt(spread + epsilon)
    return (jnp.repeat(mean, per), jnp.repeat(scale, per))


def norm_back(upstream, centred, scaled, gain, scale, members, per):
    gate = jax.nn.sigmoid(scaled)
    slope = upstream * gate * (1.0 + scaled * (1.0 - gate))
    totals = clip_totals(
        jnp.stack([jnp.sum(slope, axis=(0, 1, 2)), jnp.sum(slope * centred, axis=(0, 1, 2))])
    )
    first = jnp.repeat(jnp.sum((gain * totals[0]).reshape(-1, per), axis=1), per) / members
    second = jnp.repeat(jnp.sum((gain * totals[1]).reshape(-1, per), axis=1), per) / members
    return (scale * (slope * gain - first - centred * second), totals[1])


def tap_stack(extended, frames, height, width):
    pieces = []
    for frame_tap in range(3):
        for row_tap in range(3):
            for col_tap in range(3):
                pieces.append(
                    extended[
                        2 - frame_tap : 2 - frame_tap + frames,
                        2 - row_tap : 2 - row_tap + height,
                        2 - col_tap : 2 - col_tap + width,
                    ]
                )
    stacked = jnp.stack(pieces, axis=3)
    return stacked.reshape(frames * height * width, 27, extended.shape[3])


def rounded_up(size, unit):
    return -(-size // unit) * unit


def gathered(grad, wide):
    rows = lax.all_gather(grad, "space", axis=1, tiled=True)
    whole = lax.all_gather(rows, "tm", axis=0, tiled=True)
    return jnp.pad(whole, ((0, 2), (1, 1), (0, wide - grad.shape[2]), (0, 0)))


def channel_shares(field, wide, share, rows):
    frames, height, width, channels = field.shape
    count = channels // share
    field = jnp.pad(field, ((0, 0), (0, 0), (0, wide - width), (0, 0)))
    field = field.reshape(frames, height * wide, channels).transpose(0, 2, 1)
    field = field.reshape(frames, count, share, height * wide).transpose(1, 0, 2, 3)
    return jnp.pad(field, ((0, 0), (0, 0), (0, rows - share), (0, 0)))


def exchanged(fields):
    blocks = lax.all_to_all(fields, CLIP, 0, 0, tiled=True)
    tm, space = lax.axis_size("tm"), lax.axis_size("space")
    _, frames, rows, lanes = blocks.shape
    blocks = blocks.reshape(tm, space, frames, rows, lanes).transpose(0, 2, 3, 1, 4)
    return blocks.reshape(tm * frames, rows, space * lanes)


def delta_share(field, mean, scale, gain, padded, width, wide):
    total, rows, lanes = field.shape
    depth = padded.shape[3]
    padded = padded.reshape(padded.shape[0], -1, depth)
    columns = jnp.stack([mean, scale, gain], axis=1)

    def body(field_ref, columns_ref, padded_ref, out_ref):
        frame = pl.program_id(0)

        @pl.when(frame == 0)
        def _():
            out_ref[...] = jnp.zeros_like(out_ref)

        column = columns_ref[...]
        scaled = (field_ref[0].astype(jnp.float32) - column[:, 0:1]) * column[:, 1:2] * column[:, 2:3]
        active = (scaled * jax.nn.sigmoid(scaled)).astype(jnp.bfloat16).astype(jnp.float32)
        place = lax.broadcasted_iota(jnp.int32, active.shape, 1)
        active = jnp.where(place % wide < width, active, 0.0)
        left = jnp.concatenate(
            [pltpu.roll(active, 1, 1), active, pltpu.roll(active, lanes - 1, 1)], axis=0
        ).astype(jnp.bfloat16)
        right = jnp.concatenate(
            [
                padded_ref[frame + 2 - a, (2 - b) * wide : (2 - b) * wide + lanes, :]
                for a in range(3)
                for b in range(3)
            ],
            axis=1,
        )
        out_ref[...] += lax.dot_general(
            left, right, (((1,), (0,)), ((), ())), preferred_element_type=jnp.float32
        )

    out = pl.pallas_call(
        body,
        grid=(total,),
        in_specs=[
            pl.BlockSpec((1, rows, lanes), lambda t: (t, 0, 0)),
            pl.BlockSpec((rows, 3), lambda t: (0, 0)),
            pl.BlockSpec(padded.shape, lambda t: (0, 0, 0)),
        ],
        out_specs=pl.BlockSpec((3 * rows, 9 * depth), lambda t: (0, 0)),
        out_shape=jax.ShapeDtypeStruct((3 * rows, 9 * depth), jnp.float32),
        cost_estimate=pl.CostEstimate(
            flops=2 * total * lanes * 27 * rows * depth, bytes_accessed=4 << 20, transcendentals=0
        ),
        name="delta_share",
    )(field, columns, padded)
    return out.reshape(3, rows, 3, 3, depth).transpose(1, 2, 3, 0, 4)


def summed_over_chan(partial, half):
    if lax.axis_size("chan") != 2:
        return lax.psum_scatter(partial, "chan", scatter_dimension=3, tiled=True)
    own = lax.axis_index("chan") * half
    other = lax.ppermute(
        lax.dynamic_slice_in_dim(partial, half - own, half, 3), "chan", [(0, 1), (1, 0)]
    )
    return lax.dynamic_slice_in_dim(partial, own, half, 3) + other


def gradient_back(padded, kernel, shape):
    frames, height, width, channels = shape
    half = kernel.shape[4]
    start = (lax.axis_index("tm") * frames, lax.axis_index("space") * height, 0, 0)
    near = lax.dynamic_slice(padded, start, (frames + 2, height + 2, width, half))
    near = jnp.pad(near, ((0, 0), (0, 0), (1, 1), (0, 0)))
    taps = tap_stack(near, frames, height, width)
    partial = lax.dot_general(
        taps,
        kernel.reshape(channels, 27, half),
        (((1, 2), (1, 2)), ((), ())),
        preferred_element_type=jnp.float32,
    )
    return summed_over_chan(partial.reshape(frames, height, width, channels), half)


def shards(features, hidden, cotangent, kernel_one, kernel_two, gains):
    frames, height, width, channels = features.shape
    half = kernel_one.shape[4]
    per = channels // GROUPS
    offset = lax.axis_index("chan") * half
    members = float(frames * height * width * per * lax.axis_size(CLIP))
    share = channels // lax.axis_size(CLIP)
    rows = rounded_up(share, 8)
    wide = rounded_up(width, 32)

    def own(field):
        return lax.dynamic_slice_in_dim(field, offset, half, field.ndim - 1)

    def shared(values):
        values = lax.dynamic_slice_in_dim(values, lax.axis_index(CLIP) * share, share, 0)
        return jnp.pad(values, (0, rows - share))

    cotangent_own = own(cotangent)
    padded_two = gathered(cotangent_own, wide)
    field_one = features.astype(jnp.float32)
    field_two = hidden.astype(jnp.float32)
    totals = clip_totals(
        jnp.stack(
            [
                jnp.sum(field_one, axis=(0, 1, 2)),
                jnp.sum(field_one * field_one, axis=(0, 1, 2)),
                jnp.sum(field_two, axis=(0, 1, 2)),
                jnp.sum(field_two * field_two, axis=(0, 1, 2)),
            ]
        )
    )
    both = jnp.concatenate(
        [channel_shares(features, wide, share, rows), channel_shares(hidden, wide, share, rows)],
        axis=2,
    )
    both = exchanged(both)
    mean_one, scale_one = statistics(totals[0], totals[1], members, per)
    mean_two, scale_two = statistics(totals[2], totals[3], members, per)
    centred_one = (own(field_one) - own(mean_one)) * own(scale_one)
    scaled_one = centred_one * own(gains[0])
    centred_two = (own(field_two) - own(mean_two)) * own(scale_two)
    scaled_two = centred_two * own(gains[1])
    back_two = gradient_back(padded_two, kernel_two, features.shape)
    grad_two, weighted_two = norm_back(
        back_two, centred_two, scaled_two, own(gains[1]), own(scale_two), members, per
    )
    delta_two = delta_share(
        both[:, rows:], shared(mean_two), shared(scale_two), shared(gains[1]), padded_two, width, wide
    )
    padded_one = gathered(grad_two.astype(jnp.bfloat16), wide)
    back_one = gradient_back(padded_one, kernel_one, features.shape)
    delta_one = delta_share(
        both[:, :rows], shared(mean_one), shared(scale_one), shared(gains[0]), padded_one, width, wide
    )
    grad_one, weighted_one = norm_back(
        back_one, centred_one, scaled_one, own(gains[0]), own(scale_one), members, per
    )
    feature_grad = (cotangent_own.astype(jnp.float32) + grad_one).astype(jnp.bfloat16)
    return (
        feature_grad,
        delta_one[:share],
        delta_two[:share],
        jnp.stack([weighted_one, weighted_two]),
    )


def solution(mesh):
    placed = (
        P(("clip", "tm"), "space", None, None),
        P(("clip", "tm"), "space", None, None),
        P(("clip", "tm"), "space", None, None),
        P(None, None, None, None, "chan"),
        P(None, None, None, None, "chan"),
        P(),
    )
    return jax.shard_map(
        shards,
        mesh=mesh,
        in_specs=placed,
        out_specs=(
            P(("clip", "tm"), "space", None, "chan"),
            P(("clip", "tm", "space"), None, None, None, "chan"),
            P(("clip", "tm", "space"), None, None, None, "chan"),
            P("clip", "chan"),
        ),
        check_vma=False,
    )
```

```python
import jax
import jax.numpy as jnp
from jax import lax
from jax.experimental import pallas as pl
from jax.experimental.pallas import tpu as pltpu
from jax.sharding import PartitionSpec as P

GROUPS = 32


epsilon = 1e-06


CLIP = ("tm", "space")


def clip_totals(values):
    count = lax.axis_size(CLIP)
    if count & (count - 1):
        return lax.psum(values, CLIP)
    step = 1
    while step < count:
        values = values + lax.ppermute(values, CLIP, [(i, i ^ step) for i in range(count)])
        step *= 2
    return values


def group_sums(values, per):
    group = jnp.arange(values.shape[1]) // per
    same = (group[:, None] == group[None, :]).astype(jnp.float32)
    return jnp.dot(values, same, precision=lax.Precision.HIGHEST)


def norm_back(upstream, centred, scaled, gain, scale, members, per):
    gate = jax.nn.sigmoid(scaled)
    slope = upstream * gate * (1.0 + scaled * (1.0 - gate))
    totals = clip_totals(
        jnp.stack([jnp.sum(slope, axis=(0, 1, 2)), jnp.sum(slope * centred, axis=(0, 1, 2))])
    )
    shifts = group_sums(gain * totals, per) / members
    return (scale * (slope * gain - shifts[0] - centred * shifts[1]), totals[1])


def tap_stack(extended, frames, height, width):
    pieces = []
    for frame_tap in range(3):
        for row_tap in range(3):
            for col_tap in range(3):
                pieces.append(
                    extended[
                        2 - frame_tap : 2 - frame_tap + frames,
                        2 - row_tap : 2 - row_tap + height,
                        2 - col_tap : 2 - col_tap + width,
                    ]
                )
    stacked = jnp.stack(pieces, axis=3)
    return stacked.reshape(frames * height * width, 27, extended.shape[3])


def rounded_up(size, unit):
    return -(-size // unit) * unit


def extended(grad):
    tm, space = lax.axis_size("tm"), lax.axis_size("space")

    def moved(block, frame_step, row_step):
        route = []
        for t in range(tm):
            for s in range(space):
                if 0 <= t - frame_step and 0 <= s + row_step < space:
                    route.append((t * space + s, (t - frame_step) * space + s + row_step))
        if not route:
            return jnp.zeros_like(block)
        return lax.ppermute(block, CLIP, route)

    height = grad.shape[1]
    first, last, early = grad[:, :1], grad[:, height - 1 :], grad[:2]
    now = jnp.concatenate([moved(last, 0, 1), grad, moved(first, 0, -1)], axis=1)
    later = jnp.concatenate(
        [moved(last[:2], 1, 1), moved(early, 1, 0), moved(first[:2], 1, -1)], axis=1
    )
    joined = jnp.concatenate([now, later], axis=0)
    return jnp.pad(joined, ((0, 0), (0, 0), (1, 1), (0, 0)))


def exchanged(fields, wide, share, rows):
    kinds, frames, height, width, channels = fields.shape
    tm, space = lax.axis_size("tm"), lax.axis_size("space")
    fields = jnp.pad(fields, ((0, 0), (0, 0), (0, 0), (0, wide - width), (0, 0)))
    fields = fields.reshape(kinds, frames, height * wide, channels).transpose(0, 1, 3, 2)
    fields = fields.reshape(kinds, frames, tm * space, share, height * wide).transpose(2, 0, 1, 3, 4)
    fields = jnp.pad(fields, ((0, 0), (0, 0), (0, 0), (0, rows - share), (0, 0)))
    blocks = lax.all_to_all(fields, CLIP, 0, 0, tiled=True)
    return blocks.reshape(tm, space, kinds, frames, rows, height * wide)


def delta_share(blocks, kind, columns, grads, share, wide):
    tm, space, _, frames, rows, part = blocks.shape
    _, _, height, width, depth = grads.shape
    total, lanes = tm * frames, space * part
    tall = space * height

    def body(field_ref, columns_ref, grads_ref, out_ref, padded_ref, sum_ref):
        frame = pl.program_id(0)

        @pl.when(frame == 0)
        def _():
            sum_ref[...] = jnp.zeros_like(sum_ref)
            padded_ref[...] = jnp.zeros_like(padded_ref)
            for device in range(tm * space):
                t, s = device // space, device % space
                for f in range(frames):
                    for h in range(height):
                        row = (1 + s * height + h) * wide
                        padded_ref[t * frames + f, row : row + width, :] = grads_ref[device, f, h]

        column = columns_ref[...]
        field = jnp.concatenate([field_ref[0, s, 0, 0] for s in range(space)], axis=1)
        scaled = (field.astype(jnp.float32) - column[:, 0:1]) * column[:, 1:2] * column[:, 2:3]
        active = (scaled * jax.nn.sigmoid(scaled)).astype(jnp.bfloat16).astype(jnp.float32)
        place = lax.broadcasted_iota(jnp.int32, active.shape, 1)
        active = jnp.where(place % wide < width, active, 0.0)
        left = jnp.concatenate(
            [pltpu.roll(active, 1, 1), active, pltpu.roll(active, lanes - 1, 1)], axis=0
        ).astype(jnp.bfloat16)
        right = jnp.concatenate(
            [
                padded_ref[frame + 2 - a, (2 - b) * wide : (2 - b) * wide + lanes, :]
                for a in range(3)
                for b in range(3)
            ],
            axis=1,
        )
        sum_ref[...] += lax.dot_general(
            left, right, (((1,), (0,)), ((), ())), preferred_element_type=jnp.float32
        )

        @pl.when(frame == total - 1)
        def _():
            for a in range(3):
                for b in range(3):
                    for c in range(3):
                        column = (3 * a + b) * depth
                        out_ref[:, a, b, c, :] = sum_ref[
                            c * rows : c * rows + share, column : column + depth
                        ]

    return pl.pallas_call(
        body,
        grid=(total,),
        in_specs=[
            pl.BlockSpec(
                (1, space, 1, 1, rows, part), lambda t: (t // frames, 0, kind, t % frames, 0, 0)
            ),
            pl.BlockSpec((rows, 3), lambda t: (0, 0)),
            pl.BlockSpec(grads.shape, lambda t: (0, 0, 0, 0, 0)),
        ],
        out_specs=pl.BlockSpec((share, 3, 3, 3, depth), lambda t: (0, 0, 0, 0, 0)),
        out_shape=jax.ShapeDtypeStruct((share, 3, 3, 3, depth), jnp.float32),
        scratch_shapes=[
            pltpu.VMEM((total + 2, (tall + 2) * wide, depth), jnp.bfloat16),
            pltpu.VMEM((3 * rows, 9 * depth), jnp.float32),
        ],
        compiler_params=pltpu.CompilerParams(vmem_limit_bytes=(12 << 20) + 6 * total * tall * wide * depth),
        cost_estimate=pl.CostEstimate(
            flops=2 * total * lanes * 27 * rows * depth, bytes_accessed=4 << 20, transcendentals=0
        ),
        name="delta_share",
    )(blocks, columns, grads)


def summed_over_chan(partial, half):
    if lax.axis_size("chan") != 2:
        return lax.psum_scatter(partial, "chan", scatter_dimension=3, tiled=True)
    own = lax.axis_index("chan") * half
    other = lax.ppermute(
        lax.dynamic_slice_in_dim(partial, half - own, half, 3), "chan", [(0, 1), (1, 0)]
    )
    return lax.dynamic_slice_in_dim(partial, own, half, 3) + other


def gradient_back(grad, kernel, shape):
    frames, height, width, channels = shape
    half = kernel.shape[4]
    taps = tap_stack(extended(grad), frames, height, width)
    partial = lax.dot_general(
        taps,
        kernel.reshape(channels, 27, half),
        (((1, 2), (1, 2)), ((), ())),
        preferred_element_type=jnp.float32,
    )
    return summed_over_chan(partial.reshape(frames, height, width, channels), half)


def shards(features, hidden, cotangent, kernel_one, kernel_two, gains):
    frames, height, width, channels = features.shape
    half = kernel_one.shape[4]
    per = channels // GROUPS
    offset = lax.axis_index("chan") * half
    members = float(frames * height * width * per * lax.axis_size(CLIP))
    share = channels // lax.axis_size(CLIP)
    rows = rounded_up(share, 8)
    wide = rounded_up(width, 32)

    def own(field):
        return lax.dynamic_slice_in_dim(field, offset, half, field.ndim - 1)

    def shared(mean, scale, gain):
        values = jnp.stack([mean, scale, gain])
        values = lax.dynamic_slice_in_dim(values, lax.axis_index(CLIP) * share, share, 1)
        return jnp.pad(values.T, ((0, rows - share), (0, 0)))

    cotangent_own = own(cotangent)
    grads_two = lax.all_gather(cotangent_own, CLIP)
    both = exchanged(jnp.stack([features, hidden]), wide, share, rows)
    field_one = features.astype(jnp.float32)
    field_two = hidden.astype(jnp.float32)
    totals = clip_totals(
        jnp.stack(
            [
                jnp.sum(field_one, axis=(0, 1, 2)),
                jnp.sum(field_two, axis=(0, 1, 2)),
                jnp.sum(field_one * field_one, axis=(0, 1, 2)),
                jnp.sum(field_two * field_two, axis=(0, 1, 2)),
            ]
        )
    )
    moments = group_sums(totals, per) / members
    means = moments[:2]
    scales = lax.rsqrt(moments[2:] - means * means + epsilon)
    centred_one = (own(field_one) - own(means[0])) * own(scales[0])
    scaled_one = centred_one * own(gains[0])
    centred_two = (own(field_two) - own(means[1])) * own(scales[1])
    scaled_two = centred_two * own(gains[1])
    back_two = gradient_back(cotangent_own, kernel_two, features.shape)
    grad_two, weighted_two = norm_back(
        back_two, centred_two, scaled_two, own(gains[1]), own(scales[1]), members, per
    )
    grad_hidden = grad_two.astype(jnp.bfloat16)
    grads_one = lax.all_gather(grad_hidden, CLIP)
    delta_two = delta_share(
        both, 1, shared(means[1], scales[1], gains[1]), grads_two, share, wide
    )
    back_one = gradient_back(grad_hidden, kernel_one, features.shape)
    grad_one, weighted_one = norm_back(
        back_one, centred_one, scaled_one, own(gains[0]), own(scales[0]), members, per
    )
    delta_one = delta_share(
        both, 0, shared(means[0], scales[0], gains[0]), grads_one, share, wide
    )
    feature_grad = (cotangent_own.astype(jnp.float32) + grad_one).astype(jnp.bfloat16)
    return (feature_grad, delta_one, delta_two, jnp.stack([weighted_one, weighted_two]))


def solution(mesh):
    placed = (
        P(("clip", "tm"), "space", None, None),
        P(("clip", "tm"), "space", None, None),
        P(("clip", "tm"), "space", None, None),
        P(None, None, None, None, "chan"),
        P(None, None, None, None, "chan"),
        P(),
    )
    return jax.shard_map(
        shards,
        mesh=mesh,
        in_specs=placed,
        out_specs=(
            P(("clip", "tm"), "space", None, "chan"),
            P(("clip", "tm", "space"), None, None, None, "chan"),
            P(("clip", "tm", "space"), None, None, None, "chan"),
            P("clip", "chan"),
        ),
        check_vma=False,
    )
```

```python
import jax
import jax.numpy as jnp
from jax import lax
from jax.experimental import pallas as pl
from jax.experimental.pallas import tpu as pltpu
from jax.sharding import PartitionSpec as P

GROUPS = 32


epsilon = 1e-06


CLIP = ("tm", "space")


def clip_totals(values):
    count = lax.axis_size(CLIP)
    if count & (count - 1):
        return lax.psum(values, CLIP)
    step = 1
    while step < count:
        values = values + lax.ppermute(values, CLIP, [(i, i ^ step) for i in range(count)])
        step *= 2
    return values


def group_sums(values, per):
    group = jnp.arange(values.shape[1]) // per
    same = (group[:, None] == group[None, :]).astype(jnp.float32)
    return jnp.dot(values, same, precision=lax.Precision.HIGHEST)


def norm_back(upstream, centred, scaled, gain, scale, members, per):
    gate = jax.nn.sigmoid(scaled)
    slope = upstream * gate * (1.0 + scaled * (1.0 - gate))
    totals = clip_totals(
        jnp.stack([jnp.sum(slope, axis=(0, 1, 2)), jnp.sum(slope * centred, axis=(0, 1, 2))])
    )
    shifts = group_sums(gain * totals, per) / members
    return (scale * (slope * gain - shifts[0] - centred * shifts[1]), totals[1])


def tap_stack(extended, frames, height, width):
    pieces = []
    for frame_tap in range(3):
        for row_tap in range(3):
            for col_tap in range(3):
                pieces.append(
                    extended[
                        2 - frame_tap : 2 - frame_tap + frames,
                        2 - row_tap : 2 - row_tap + height,
                        2 - col_tap : 2 - col_tap + width,
                    ]
                )
    stacked = jnp.stack(pieces, axis=3)
    return stacked.reshape(frames * height * width, 27, extended.shape[3])


def rounded_up(size, unit):
    return -(-size // unit) * unit


def extended(grad):
    tm, space = lax.axis_size("tm"), lax.axis_size("space")

    def moved(block, frame_step, row_step):
        route = []
        for t in range(tm):
            for s in range(space):
                if 0 <= t - frame_step and 0 <= s + row_step < space:
                    route.append((t * space + s, (t - frame_step) * space + s + row_step))
        if not route:
            return jnp.zeros_like(block)
        return lax.ppermute(block, CLIP, route)

    height = grad.shape[1]
    first, last, early = grad[:, :1], grad[:, height - 1 :], grad[:2]
    now = jnp.concatenate([moved(last, 0, 1), grad, moved(first, 0, -1)], axis=1)
    later = jnp.concatenate(
        [moved(last[:2], 1, 1), moved(early, 1, 0), moved(first[:2], 1, -1)], axis=1
    )
    joined = jnp.concatenate([now, later], axis=0)
    return jnp.pad(joined, ((0, 0), (0, 0), (1, 1), (0, 0)))


def exchanged(fields, wide, share, rows):
    kinds, frames, height, width, channels = fields.shape
    tm, space = lax.axis_size("tm"), lax.axis_size("space")
    fields = jnp.pad(fields, ((0, 0), (0, 0), (0, 0), (0, wide - width), (0, 0)))
    fields = fields.reshape(kinds, frames, height * wide, channels).transpose(0, 1, 3, 2)
    fields = fields.reshape(kinds, frames, tm * space, share, height * wide).transpose(2, 0, 1, 3, 4)
    fields = jnp.pad(fields, ((0, 0), (0, 0), (0, 0), (0, rows - share), (0, 0)))
    blocks = lax.all_to_all(fields, CLIP, 0, 0, tiled=True)
    return blocks.reshape(tm, space, kinds, frames, rows, height * wide)


def delta_share(blocks, kind, columns, grads, share, wide):
    tm, space, _, frames, rows, part = blocks.shape
    _, _, height, width, depth = grads.shape
    total, lanes = tm * frames, space * part
    tall = space * height

    def body(field_ref, columns_ref, grads_ref, out_ref, padded_ref, sum_ref):
        frame = pl.program_id(0)

        @pl.when(frame == 0)
        def _():
            sum_ref[...] = jnp.zeros_like(sum_ref)
            padded_ref[...] = jnp.zeros_like(padded_ref)
            for device in range(tm * space):
                t, s = device // space, device % space
                for f in range(frames):
                    for h in range(height):
                        row = (1 + s * height + h) * wide
                        padded_ref[t * frames + f, row : row + width, :] = grads_ref[device, f, h]

        column = columns_ref[...]
        field = jnp.concatenate([field_ref[0, s, 0, 0] for s in range(space)], axis=1)
        scaled = (field.astype(jnp.float32) - column[:, 0:1]) * column[:, 1:2] * column[:, 2:3]
        active = (scaled * jax.nn.sigmoid(scaled)).astype(jnp.bfloat16).astype(jnp.float32)
        place = lax.broadcasted_iota(jnp.int32, active.shape, 1)
        active = jnp.where(place % wide < width, active, 0.0)
        left = jnp.concatenate(
            [pltpu.roll(active, 1, 1), active, pltpu.roll(active, lanes - 1, 1)], axis=0
        ).astype(jnp.bfloat16)
        right = jnp.concatenate(
            [
                padded_ref[frame + 2 - a, (2 - b) * wide : (2 - b) * wide + lanes, :]
                for a in range(3)
                for b in range(3)
            ],
            axis=1,
        )
        sum_ref[...] += lax.dot_general(
            left, right, (((1,), (0,)), ((), ())), preferred_element_type=jnp.float32
        )

        @pl.when(frame == total - 1)
        def _():
            for a in range(3):
                for b in range(3):
                    for c in range(3):
                        column = (3 * a + b) * depth
                        out_ref[:, a, b, c, :] = sum_ref[
                            c * rows : c * rows + share, column : column + depth
                        ]

    return pl.pallas_call(
        body,
        grid=(total,),
        in_specs=[
            pl.BlockSpec(
                (1, space, 1, 1, rows, part), lambda t: (t // frames, 0, kind, t % frames, 0, 0)
            ),
            pl.BlockSpec((rows, 3), lambda t: (0, 0)),
            pl.BlockSpec(grads.shape, lambda t: (0, 0, 0, 0, 0)),
        ],
        out_specs=pl.BlockSpec((share, 3, 3, 3, depth), lambda t: (0, 0, 0, 0, 0)),
        out_shape=jax.ShapeDtypeStruct((share, 3, 3, 3, depth), jnp.float32),
        scratch_shapes=[
            pltpu.VMEM((total + 2, (tall + 2) * wide, depth), jnp.bfloat16),
            pltpu.VMEM((3 * rows, 9 * depth), jnp.float32),
        ],
        compiler_params=pltpu.CompilerParams(vmem_limit_bytes=(12 << 20) + 6 * total * tall * wide * depth),
        cost_estimate=pl.CostEstimate(
            flops=2 * total * lanes * 27 * rows * depth, bytes_accessed=4 << 20, transcendentals=0
        ),
        name="delta_share",
    )(blocks, columns, grads)


def summed_over_chan(partial, half):
    if lax.axis_size("chan") != 2:
        return lax.psum_scatter(partial, "chan", scatter_dimension=3, tiled=True)
    own = lax.axis_index("chan") * half
    other = lax.ppermute(
        lax.dynamic_slice_in_dim(partial, half - own, half, 3), "chan", [(0, 1), (1, 0)]
    )
    return lax.dynamic_slice_in_dim(partial, own, half, 3) + other


def gradient_back(grad, kernel, shape):
    frames, height, width, channels = shape
    half = kernel.shape[4]
    taps = tap_stack(extended(grad), frames, height, width)
    partial = lax.dot_general(
        taps,
        kernel.reshape(channels, 27, half),
        (((1, 2), (1, 2)), ((), ())),
        preferred_element_type=jnp.float32,
    )
    return summed_over_chan(partial.reshape(frames, height, width, channels), half)


def shards(features, hidden, cotangent, kernel_one, kernel_two, gains):
    frames, height, width, channels = features.shape
    half = kernel_one.shape[4]
    per = channels // GROUPS
    offset = lax.axis_index("chan") * half
    members = float(frames * height * width * per * lax.axis_size(CLIP))
    share = channels // lax.axis_size(CLIP)
    rows = rounded_up(share, 8)
    wide = rounded_up(width, 32)

    def own(field):
        return lax.dynamic_slice_in_dim(field, offset, half, field.ndim - 1)

    def shared(mean, scale, gain):
        values = jnp.stack([mean, scale, gain])
        values = lax.dynamic_slice_in_dim(values, lax.axis_index(CLIP) * share, share, 1)
        return jnp.pad(values.T, ((0, rows - share), (0, 0)))

    cotangent_own = own(cotangent)
    grads_two = lax.all_gather(cotangent_own, CLIP)
    both = exchanged(jnp.stack([features, hidden]), wide, share, rows)
    field_one = features.astype(jnp.float32)
    field_two = hidden.astype(jnp.float32)
    totals = clip_totals(
        jnp.stack(
            [
                jnp.sum(field_one, axis=(0, 1, 2)),
                jnp.sum(field_two, axis=(0, 1, 2)),
                jnp.sum(field_one * field_one, axis=(0, 1, 2)),
                jnp.sum(field_two * field_two, axis=(0, 1, 2)),
            ]
        )
    )
    moments = group_sums(totals, per) / members
    means = moments[:2]
    scales = lax.rsqrt(moments[2:] - means * means + epsilon)
    centred_one = (own(field_one) - own(means[0])) * own(scales[0])
    scaled_one = centred_one * own(gains[0])
    centred_two = (own(field_two) - own(means[1])) * own(scales[1])
    scaled_two = centred_two * own(gains[1])
    back_two = gradient_back(cotangent_own, kernel_two, features.shape)
    grad_two, weighted_two = norm_back(
        back_two, centred_two, scaled_two, own(gains[1]), own(scales[1]), members, per
    )
    grad_hidden = grad_two.astype(jnp.bfloat16)
    grads_one = lax.all_gather(grad_hidden, CLIP)
    delta_two = delta_share(
        both, 1, shared(means[1], scales[1], gains[1]), grads_two, share, wide
    )
    back_one = gradient_back(grad_hidden, kernel_one, features.shape)
    back_one, delta_two = lax.optimization_barrier((back_one, delta_two))
    grad_one, weighted_one = norm_back(
        back_one, centred_one, scaled_one, own(gains[0]), own(scales[0]), members, per
    )
    delta_one = delta_share(
        both, 0, shared(means[0], scales[0], gains[0]), grads_one, share, wide
    )
    feature_grad = (cotangent_own.astype(jnp.float32) + grad_one).astype(jnp.bfloat16)
    return (feature_grad, delta_one, delta_two, jnp.stack([weighted_one, weighted_two]))


def solution(mesh):
    placed = (
        P(("clip", "tm"), "space", None, None),
        P(("clip", "tm"), "space", None, None),
        P(("clip", "tm"), "space", None, None),
        P(None, None, None, None, "chan"),
        P(None, None, None, None, "chan"),
        P(),
    )
    return jax.shard_map(
        shards,
        mesh=mesh,
        in_specs=placed,
        out_specs=(
            P(("clip", "tm"), "space", None, "chan"),
            P(("clip", "tm", "space"), None, None, None, "chan"),
            P(("clip", "tm", "space"), None, None, None, "chan"),
            P("clip", "chan"),
        ),
        check_vma=False,
    )
```
